32 devices in a mesh: dp: 8 (over z, y), tensor: 4 (over x, core).
Axes of the slice: x: 2, y: 2, z: 4, core: 2. Of those that a mesh axis runs over, the one named last changes fastest.
Arguments:
- hidden: bfloat16 [4096, 5120], P('dp'), may hold values from -48 to 48
- head_weight: bfloat16 [5120, 4096], P(None, 'tensor'), may hold values from -0.069877124 to 0.069877124
- token_ids: int32 [4096], P('dp'), may hold values from 0 to 4095
- old_logprob: float32 [4096], P('dp'), may hold values from -12.5 to 0.3
- rewards: int32 [64], P('dp'), may hold values from 0 to 1, as said below
- lengths: int32 [64], P('dp'), may hold values from 1 to 64, as said below
- group_ids: int32 [64], P('dp'), may hold values from 0 to 3, as said below
- loss_scale: float32 [], replicated, may hold values from 4096 to 16384
Outputs:
- loss: float32 [], replicated
- grad_hidden: float32 [4096, 5120], P('dp', 'tensor')
- grad_weight: float32 [5120, 4096], P('dp', 'tensor')
The draws below stay inside these ranges and needn't reach their ends.
Inputs may be any that keep to these rules, and one draw needn't show every extreme that they name: `group_ids`: each group number names exactly 16 rollouts. `rewards`: some group holds both a 0 and a 1. `lengths`: some index of dp holds only rollouts of length 64 whose prompts hold both a 0 and a 1.
All inputs are finite; a program needn't handle non-finite values.
Results may differ from the reference program's by a relative error of at most 0.003.
Values may be sent and summed in bfloat16 or wider, within the bound.
A program may use at most 192 MiB of HBM per device.

```python
import math
import jax
import jax.numpy as jnp
from jax import lax

D = 5120
ROLL_DEV = 8
RESP = 64
GROUP = 16
VOCAB = 4096
ROLLOUTS = 64
GROUPS = 4
TOKENS = 4096


def weight_table(key):
    branch_key = jax.random.fold_in(key, 101)
    weight_grid = jnp.clip(jax.random.normal(branch_key, (D, VOCAB), jnp.float32), -5.0, 5.0)
    return weight_grid * D ** (-0.5)


def token_table(key):
    branch_key = jax.random.fold_in(key, 202)
    first_draw = jax.random.randint(jax.random.fold_in(branch_key, 1), (TOKENS,), 0, VOCAB)
    second_draw = jax.random.randint(jax.random.fold_in(branch_key, 2), (TOKENS,), 1, VOCAB + 1)
    return (first_draw * second_draw // VOCAB).astype(jnp.int32)


def group_table(key):
    branch_key = jax.random.fold_in(key, 505)
    device_count = ROLLOUTS // ROLL_DEV
    forced_device = jax.random.randint(jax.random.fold_in(branch_key, 5), (), 0, device_count)
    roll_index = jnp.arange(ROLLOUTS, dtype=jnp.int32)
    in_forced = roll_index // ROLL_DEV == forced_device
    order_key = jax.random.permutation(jax.random.fold_in(branch_key, 1), ROLLOUTS).astype(jnp.int32)
    order_key = order_key + jnp.where(in_forced, 0, ROLLOUTS).astype(jnp.int32)
    ordering = jnp.argsort(order_key, stable=True).astype(jnp.int32)
    rank = jnp.argsort(ordering, stable=True).astype(jnp.int32)
    rank_group = (rank // GROUP).astype(jnp.int32)
    group_of = rank_group
    group_kind = jax.random.randint(jax.random.fold_in(branch_key, 2), (GROUPS,), 0, 4)
    dead_kind = jax.random.randint(jax.random.fold_in(branch_key, 3), (), 0, 2)
    group_index = jnp.arange(GROUPS, dtype=jnp.int32)
    group_kind = jnp.where(group_index == 0, 2, jnp.where(group_index == 1, dead_kind, group_kind))
    group_kind = jnp.where(group_index == GROUPS - 1, 3, group_kind)
    coin_flip = jax.random.randint(jax.random.fold_in(branch_key, 4), (ROLLOUTS,), 0, 2)
    slot_in_group = rank % GROUP
    roll_kind = group_kind[rank_group]
    mixed = jnp.where(slot_in_group == 0, 1, jnp.where(slot_in_group == 1, 0, coin_flip))
    reward_values = jnp.where(roll_kind == 0, 0, jnp.where(roll_kind == 1, 1, mixed))
    return (group_of, reward_values.astype(jnp.int32), in_forced)


def draw_head_weight(key, part):
    return weight_table(key).astype(jnp.bfloat16)


def draw_token_ids(key, part):
    return token_table(key)


def draw_group_ids(key, part):
    return group_table(key)[0]


def draw_rewards(key, part):
    return group_table(key)[1]


def draw_lengths(key, part):
    in_forced = group_table(key)[2]
    random_lengths = jax.random.randint(jax.random.fold_in(key, 707), (ROLLOUTS,), 1, RESP + 1)
    return jnp.where(in_forced, RESP, random_lengths).astype(jnp.int32)


def draw_hidden(key, part):
    branch_key = jax.random.fold_in(key, 303)
    values_out = jnp.clip(jax.random.normal(branch_key, (TOKENS, D), jnp.float32), -5.0, 5.0)
    return values_out.astype(jnp.bfloat16)


def draw_old_logprob(key, part):
    branch_key = jax.random.fold_in(key, 404)
    values_out = -9.5 + jnp.clip(jax.random.normal(branch_key, (TOKENS,), jnp.float32), -2.5, 2.5)
    return values_out


def setup_inputs(seed: int = 0) -> dict:
    arg_keys = jax.random.split(jax.random.key(seed), 9)
    hidden = draw_hidden(jax.random.fold_in(arg_keys[8], 71), 0)
    head_weight = draw_head_weight(jax.random.fold_in(arg_keys[8], 71), 0)
    token_ids = draw_token_ids(jax.random.fold_in(arg_keys[8], 71), 0)
    old_logprob = draw_old_logprob(jax.random.fold_in(arg_keys[8], 71), 0)
    rewards = draw_rewards(jax.random.fold_in(arg_keys[8], 71), 0)
    lengths = draw_lengths(jax.random.fold_in(arg_keys[8], 71), 0)
    group_ids = draw_group_ids(jax.random.fold_in(arg_keys[8], 71), 0)
    loss_scale = jnp.clip(jnp.exp(jax.random.uniform(arg_keys[7], (), jnp.float32, math.log(4096.0), math.log(16384.0))), 4096.0, 16384.0)
    return {"hidden": hidden, "head_weight": head_weight, "token_ids": token_ids, "old_logprob": old_logprob, "rewards": rewards, "lengths": lengths, "group_ids": group_ids, "loss_scale": loss_scale}


clip_low = 0.2
clip_high = 0.28

def group_terms(member, group_wins, reward_float):
    group_alive = jnp.logical_and(group_wins > 0.5, group_wins < GROUP - 0.5).astype(jnp.float32)
    center = group_wins / GROUP
    spread = jnp.where(group_alive > 0.5, jnp.sqrt(group_wins * (GROUP - group_wins)) / GROUP, 1.0)
    roll_alive = lax.optimization_barrier(jnp.sum(member * group_alive[None, :], axis=1))
    roll_center = lax.optimization_barrier(jnp.sum(member * center[None, :], axis=1))
    roll_spread = lax.optimization_barrier(jnp.sum(member * spread[None, :], axis=1))
    advantage = roll_alive * (reward_float - roll_center) / roll_spread
    return (group_alive, roll_alive, advantage)

def policy_terms(log_prob, old_rows, adv_rows, weight_rows, factor):
    prob_ratio = jnp.exp(log_prob - old_rows)
    clipped = jnp.clip(prob_ratio, 1.0 - clip_low, 1.0 + clip_high)
    token_loss = -jnp.minimum(prob_ratio * adv_rows, clipped * adv_rows)
    active = prob_ratio * adv_rows <= clipped * adv_rows
    coefficient = jnp.where(active, -adv_rows * prob_ratio, 0.0) * weight_rows * factor
    return (token_loss, coefficient)

def reference(hidden, head_weight, token_ids, old_logprob, rewards, lengths, group_ids, loss_scale):
    member = (group_ids[:, None] == jnp.arange(GROUPS, dtype=jnp.int32)[None, :]).astype(jnp.float32)
    reward_float = rewards.astype(jnp.float32)
    length_float = lengths.astype(jnp.float32)
    group_wins = lax.optimization_barrier(jnp.sum(member * reward_float[:, None], axis=0))
    group_alive, roll_alive, advantage = group_terms(member, group_wins, reward_float)
    token_count = jnp.sum(roll_alive * length_float)
    divisor = jnp.maximum(token_count, 1.0)
    factor = loss_scale / divisor
    position = jnp.arange(RESP, dtype=jnp.int32)
    inside = (position[None, :] < lengths[:, None]).astype(jnp.float32)
    token_weight = (roll_alive[:, None] * inside).reshape(TOKENS)
    token_adv = jnp.broadcast_to(advantage[:, None], (ROLLOUTS, RESP)).reshape(TOKENS)
    block_rows = math.gcd(TOKENS, 1024)
    block_count = TOKENS // block_rows
    column = jnp.arange(VOCAB, dtype=jnp.int32)[None, :]

    def one_block(carried, inputs):
        grad_table, loss_sum = carried
        row_hidden, row_tokens, row_old, row_weight, row_adv = inputs
        logits = jnp.dot(row_hidden, head_weight, preferred_element_type=jnp.float32)
        row_top = lax.optimization_barrier(jnp.max(logits, axis=1))
        shifted = jnp.exp(logits - row_top[:, None])
        row_total = lax.optimization_barrier(jnp.sum(shifted, axis=1))
        is_target = column == row_tokens[:, None]
        target = lax.optimization_barrier(jnp.sum(jnp.where(is_target, logits, 0.0), axis=1))
        softmax_rows = shifted / row_total[:, None]
        log_prob = target - row_top - jnp.log(row_total)
        token_loss, coefficient = policy_terms(log_prob, row_old, row_adv, row_weight, factor)
        logit_grad = (coefficient[:, None] * (is_target.astype(jnp.float32) - softmax_rows)).astype(jnp.bfloat16)
        grad_rows = jnp.dot(logit_grad, head_weight.T, preferred_element_type=jnp.float32)
        grad_table = grad_table + jnp.dot(row_hidden.T, logit_grad, preferred_element_type=jnp.float32)
        return ((grad_table, loss_sum + jnp.sum(row_weight * token_loss)), grad_rows)
    inputs = (hidden.reshape(block_count, block_rows, D), token_ids.reshape(block_count, block_rows), old_logprob.reshape(block_count, block_rows), token_weight.reshape(block_count, block_rows), token_adv.reshape(block_count, block_rows))
    initial = (jnp.zeros((D, VOCAB), jnp.float32), jnp.zeros((), jnp.float32))
    final_state, stacked = lax.scan(one_block, initial, inputs)
    grad_table, loss_sum = final_state
    return (loss_sum / divisor, stacked.reshape(TOKENS, D), grad_table)
```

```python
import functools

import jax
import jax.numpy as jnp
from jax import lax
from jax.experimental import pallas as pl
from jax.experimental.pallas import tpu as pltpu
from jax.sharding import PartitionSpec as P

GROUP = 16
clip_low = 0.2
clip_high = 0.28
MESH = pl.DeviceIdType.MESH
F32 = jnp.float32
BF16 = jnp.bfloat16


def kernel(cfg, hidden, hsrc, w, rows, info, loss_o, gh_o, gw_o,
           hid_v, w_v, logits, cols, stats, info_all, loss_all, lg_all, hcol, rs_recv,
           ld, s_info, r_info, s_hid, r_hid, s_x, r_x, s_d, r_d, s_st, r_st,
           s_loss, r_loss, s_rs, r_rs, s_a, s_b, r_lg):
    dp, T, nA, nB, sliced = cfg
    R, D = hid_v.shape
    V = w_v.shape[1]
    Q = R // T
    C = D // dp
    CT = D // T
    nX = T // 2
    NK = 8
    KC = D // NK
    me = lax.axis_index("dp")
    t = lax.axis_index("tensor")
    a, b = me // nB, me % nB
    x, c = t // 2, t % 2

    def rcopy(src, dst, ss, rs, dev):
        return pltpu.make_async_remote_copy(
            src_ref=src, dst_ref=dst, send_sem=ss, recv_sem=rs, device_id=dev, device_id_type=MESH
        )

    def load_h(k):
        s = pl.ds(pl.multiple_of(k * KC, KC), KC)
        return pltpu.make_async_copy(hidden.at[:, s], hid_v.at[:, s], ld.at[0, k])

    def load_w(k):
        s = pl.ds(pl.multiple_of(k * KC, KC), KC)
        return pltpu.make_async_copy(w.at[s], w_v.at[s], ld.at[1, k])

    for k in range(NK):
        load_h(k).start()
        load_w(k).start()

    barrier = pltpu.get_barrier_semaphore()
    for d in range(1, dp):
        pl.semaphore_signal(barrier, inc=1, device_id={"dp": (me + d) % dp}, device_id_type=MESH)
    for d in range(1, T):
        pl.semaphore_signal(barrier, inc=1, device_id={"tensor": (t + d) % T}, device_id_type=MESH)
    pl.semaphore_wait(barrier, dp - 1 + T - 1)

    def qrows(q):
        return pl.ds(pl.multiple_of(q * Q, Q), Q)

    def hslice(j):
        if sliced:
            return hsrc.at[qrows(t), pl.ds(pl.multiple_of(j * C, C), C)]
        return hsrc.at[j, qrows(t), :]

    def c_info(d):
        j = (me + d) % dp
        return rcopy(info, info_all.at[me], s_info.at[d], r_info.at[me], {"dp": j})

    def c_hid(d):
        j = (me + d) % dp
        return rcopy(hslice(j), hcol.at[me, qrows(t), :], s_hid.at[d], r_hid.at[me], {"dp": j})

    for d in range(1, dp):
        c_info(d).start()
    for d in range(1, dp):
        c_hid(d).start()
    own_hid = pltpu.make_async_copy(hslice(me), hcol.at[me, qrows(t), :], s_hid.at[0])
    own_hid.start()
    info_all[me] = info[...]

    pad = jnp.zeros((128 - rows.shape[0], R), F32)
    cols[...] = jnp.transpose(jnp.concatenate([rows[...], pad], axis=0))

    logits[...] = jnp.zeros_like(logits)

    @pl.loop(0, NK)
    def _(k):
        s = pl.ds(pl.multiple_of(k * KC, KC), KC)
        load_h(k).wait()
        load_w(k).wait()
        logits[...] += jnp.dot(hid_v[:, s], w_v[s, :], preferred_element_type=F32)

    RC = 32
    lane = lax.broadcasted_iota(jnp.int32, (RC, 128), 1)
    vcol = lax.broadcasted_iota(jnp.int32, (RC, V), 1).astype(F32) + (t * V).astype(F32)

    @pl.loop(0, R // RC)
    def _(n):
        r = pl.ds(pl.multiple_of(n * RC, RC), RC)
        lo = logits[r, :]
        tok = cols[r, 0:1]
        top = jnp.max(lo, axis=1, keepdims=True)
        target = jnp.sum(jnp.where(vcol == tok, lo, 0.0), axis=1, keepdims=True)
        e = jnp.exp(lo - top)
        total = jnp.sum(e, axis=1, keepdims=True)
        logits[r, :] = e
        cols[r, :] = jnp.where(
            lane == 0, tok, jnp.where(lane == 1, top, jnp.where(lane == 2, total, jnp.where(lane == 3, target, 0.0)))
        )

    stats[t] = jnp.transpose(cols[...])[0:8, :]

    def c_st(d):
        return rcopy(stats.at[t], stats.at[t], s_st.at[d], r_st.at[t], {"tensor": (t + d) % T})

    for d in range(1, T):
        c_st(d).start()
    for d in range(1, dp):
        i = (me + d) % dp
        rcopy(info, info_all.at[i], s_info.at[d], r_info.at[i], {"dp": i}).wait_recv()
    wins2 = info_all[0]
    for i in range(1, dp):
        wins2 = wins2 + info_all[i]
    G8 = info.shape[0] - 8
    wins = wins2[0:G8, 0:1]
    lens = wins2[0:G8, 1:2]
    alive = jnp.logical_and(wins > 0.5, wins < GROUP - 0.5).astype(F32)
    center = wins / GROUP
    spread = jnp.where(alive > 0.5, jnp.sqrt(wins * (GROUP - wins)) / GROUP, 1.0)
    token_count = jnp.sum(alive * lens, axis=0, keepdims=True)
    divisor = jnp.maximum(token_count, 1.0)
    factor = info[G8 : G8 + 1, 0:1] / divisor
    old = rows[1:2, :]
    gid = rows[2:3, :]
    rew = rows[3:4, :]
    inside = rows[4:5, :]
    member = (lax.broadcasted_iota(jnp.int32, (G8, R), 0).astype(F32) == gid).astype(F32)
    roll_alive = jnp.sum(member * alive, axis=0, keepdims=True)
    roll_center = jnp.sum(member * center, axis=0, keepdims=True)
    roll_spread = jnp.sum(member * spread, axis=0, keepdims=True)
    adv = roll_alive * (rew - roll_center) / roll_spread
    weight = roll_alive * inside

    for d in range(1, T):
        i = (t + d) % T
        rcopy(stats.at[i], stats.at[i], s_st.at[d], r_st.at[i], {"tensor": i}).wait_recv()
    top = stats[0, 1:2, :]
    for i in range(1, T):
        top = jnp.maximum(top, stats[i, 1:2, :])
    total = jnp.zeros_like(top)
    target = jnp.zeros_like(top)
    for i in range(T):
        total = total + stats[i, 2:3, :] * jnp.exp(stats[i, 1:2, :] - top)
        target = target + stats[i, 3:4, :]
    log_prob = target - top - jnp.log(total)
    ratio = jnp.exp(log_prob - old)
    clipped = jnp.clip(ratio, 1.0 - clip_low, 1.0 + clip_high)
    token_loss = -jnp.minimum(ratio * adv, clipped * adv)
    active = ratio * adv <= clipped * adv
    coef = jnp.where(active, -adv * ratio, 0.0) * weight * factor
    mytop = stats[t][1:2, :]
    scale = jnp.exp(mytop - top) / total
    loss_all[me] = jnp.broadcast_to(jnp.sum(weight * token_loss, axis=1, keepdims=True), (8, 128))
    cols[...] = jnp.transpose(
        jnp.concatenate([rows[0:1, :], coef, scale, jnp.zeros((125, R), F32)], axis=0)
    )

    @pl.loop(0, R // RC)
    def _(n):
        r = pl.ds(pl.multiple_of(n * RC, RC), RC)
        hit = jnp.where(vcol == cols[r, 0:1], 1.0, 0.0)
        lg_all[me, r, :] = (cols[r, 1:2] * (hit - logits[r, :] * cols[r, 2:3])).astype(BF16)

    def c_up(j):
        return rcopy(lg_all.at[j], lg_all.at[j], s_a.at[0, j], r_lg.at[j], {"dp": me + nB})

    def c_down(j):
        return rcopy(lg_all.at[j], lg_all.at[j], s_a.at[1, j], r_lg.at[j], {"dp": me - nB})

    def c_b(j, d):
        return rcopy(lg_all.at[j], lg_all.at[j], s_b.at[d, j], r_lg.at[j], {"dp": a * nB + (b + d) % nB})

    def recv_lg(j):
        rcopy(lg_all.at[j], lg_all.at[j], s_a.at[0, j], r_lg.at[j], {"dp": (me + 1) % dp}).wait_recv()

    def send_b(j):
        for d in range(1, nB):
            c_b(j, d).start()

    @pl.when(a < nA - 1)
    def _():
        c_up(me).start()

    @pl.when(a > 0)
    def _():
        c_down(me).start()

    send_b(me)

    def c_loss(d):
        return rcopy(loss_all.at[me], loss_all.at[me], s_loss.at[d], r_loss.at[me], {"dp": (me + d) % dp})

    for d in range(1, dp):
        c_loss(d).start()

    GC = 640 if CT % 640 == 0 else CT
    per = CT // GC

    def gh_dot(col0):
        return lax.dot_general(
            lg_all[me], w_v[pl.ds(col0, GC), :], (((1,), (1,)), ((), ())), preferred_element_type=F32
        )

    @pl.loop(0, (T - 1) * per)
    def _(n):
        peer = (t + 1 + n // per) % T
        col0 = pl.multiple_of(peer * CT + (n % per) * GC, GC)
        hid_v[:, pl.ds(col0, GC)] = gh_dot(col0).astype(BF16)

    own_hid.wait()
    for d in range(1, dp):
        i = (me + d) % dp
        rcopy(hslice(i), hcol.at[i, qrows(t), :], s_hid.at[d], r_hid.at[i], {"dp": i}).wait_recv()

    def c_x(d):
        q = hcol.at[:, qrows(t), :]
        return rcopy(q, q, s_x.at[d], r_x.at[x], {"tensor": ((x + d) % nX) * 2 + c})

    def c_d(xx):
        q = hcol.at[:, qrows(2 * xx + c), :]
        return rcopy(q, q, s_d.at[xx], r_d.at[xx], {"tensor": 2 * x + 1 - c})

    for d in range(1, nX):
        c_x(d).start()
    c_d(x).start()

    def c_rs(d):
        peer = (t + d) % T
        return rcopy(
            hid_v.at[:, pl.ds(pl.multiple_of(peer * CT, CT), CT)],
            rs_recv.at[t], s_rs.at[d], r_rs.at[t], {"tensor": peer},
        )

    for d in range(1, T):
        c_rs(d).start()

    @pl.loop(0, per)
    def _(n):
        off = pl.multiple_of(n * GC, GC)
        gh_o[:, pl.ds(off, GC)] = gh_dot(pl.multiple_of(t * CT + off, GC))

    def relay(s):
        @pl.when(a >= s)
        def _():
            j = me - s * nB
            recv_lg(j)

            @pl.when(a < nA - 1)
            def _():
                c_up(j).start()

            send_b(j)

        @pl.when(a + s < nA)
        def _():
            j = me + s * nB
            recv_lg(j)

            @pl.when(a > 0)
            def _():
                c_down(j).start()

            send_b(j)

    def gw_add(j):
        gw_o[...] += lax.dot_general(
            hcol[j], lg_all[j], (((0,), (0,)), ((), ())), preferred_element_type=F32
        )

    gw_o[...] = jnp.zeros_like(gw_o)

    def add_steps(items):
        for s, d in items:
            @pl.loop(0, 1 if s == 0 else 2)
            def _(k):
                aa = a + (2 * k - 1) * s
                j = aa * nB + (b + d) % nB

                @pl.when(jnp.logical_and(aa >= 0, aa < nA))
                def _():
                    if d > 0:
                        recv_lg(j)
                    gw_add(j)

    relay(1)
    relay(2)
    for d in range(1, nX):
        xx = (x + d) % nX
        q = hcol.at[:, qrows(2 * xx + c), :]
        rcopy(q, q, s_x.at[d], r_x.at[xx], {"tensor": 2 * xx + c}).wait_recv()
        c_d(xx).start()
    for xx in range(nX):
        q = hcol.at[:, qrows(2 * xx + 1 - c), :]
        rcopy(q, q, s_d.at[xx], r_d.at[xx], {"tensor": 2 * x + 1 - c}).wait_recv()
    add_steps([(0, 0), (1, 0), (2, 0)] + [(0, d) for d in range(1, nB)])
    for s in range(3, nA):
        relay(s)
        add_steps([(s, 0)])
    for s in range(1, nA - 1):
        add_steps([(s, d) for d in range(1, nB)])

    for d in range(1, T):
        i = (t + d) % T
        rcopy(hid_v.at[:, pl.ds(0, CT)], rs_recv.at[i], s_rs.at[d], r_rs.at[i], {"tensor": i}).wait_recv()

    @pl.loop(0, R // RC)
    def _(n):
        r = pl.ds(pl.multiple_of(n * RC, RC), RC)
        acc = gh_o[r, :]
        for d in range(1, T):
            acc = acc + rs_recv[(t + d) % T, r, :].astype(F32)
        gh_o[r, :] = acc

    for d in range(1, dp):
        i = (me + d) % dp
        rcopy(loss_all.at[i], loss_all.at[i], s_loss.at[d], r_loss.at[i], {"dp": i}).wait_recv()
    loss = loss_all[0]
    for i in range(1, dp):
        loss = loss + loss_all[i]
    loss_o[...] = loss / divisor

    add_steps([(nA - 1, d) for d in range(1, nB)])

    for d in range(1, dp):
        c_info(d).wait_send()
        c_hid(d).wait_send()
        c_loss(d).wait_send()
    for d in range(1, T):
        c_st(d).wait_send()
        c_rs(d).wait_send()
    for d in range(1, nX):
        c_x(d).wait_send()
    for xx in range(nX):
        c_d(xx).wait_send()
    for s in range(nA):
        @pl.when(a >= s)
        def _():
            j = me - s * nB

            @pl.when(a < nA - 1)
            def _():
                c_up(j).wait_send()

            for d in range(1, nB):
                c_b(j, d).wait_send()

        @pl.when(a + s < nA)
        def _():
            j = me + s * nB

            @pl.when(a > 0)
            def _():
                c_down(j).wait_send()

            if s > 0:
                for d in range(1, nB):
                    c_b(j, d).wait_send()


def shards(hidden, head_weight, token_ids, old_logprob, rewards, lengths, group_ids, loss_scale):
    R, D = hidden.shape
    V = head_weight.shape[1]
    rolls = rewards.shape[0]
    dp = lax.axis_size("dp")
    T = lax.axis_size("tensor")
    nA = 4 if dp % 4 == 0 else dp
    nB = dp // nA
    groups = rolls * dp // GROUP
    G8 = -(-groups // 8) * 8
    C = D // dp
    sliced = C % 128 == 0
    response = R // rolls
    member = (group_ids[None, :] == jnp.arange(G8, dtype=jnp.int32)[:, None]).astype(F32)
    wins = jnp.sum(member * rewards.astype(F32)[None, :], axis=1)
    lens = jnp.sum(member * lengths.astype(F32)[None, :], axis=1)
    lane = jnp.arange(128)[None, :]
    info = jnp.where(lane == 0, wins[:, None], jnp.where(lane == 1, lens[:, None], 0.0))
    info = jnp.concatenate([info, jnp.full((8, 128), 1.0, F32) * loss_scale], axis=0)
    inside = (jnp.arange(response, dtype=jnp.int32)[None, :] < lengths[:, None]).astype(F32).reshape(R)
    spread = lambda v: jnp.broadcast_to(v.astype(F32)[:, None], (rolls, response)).reshape(R)
    zero = jnp.zeros((R,), F32)
    rows = jnp.stack(
        [token_ids.astype(F32), old_logprob, spread(group_ids), spread(rewards), inside, zero, zero, zero]
    )
    if sliced:
        hsrc = hidden
    else:
        hsrc = jnp.transpose(hidden.reshape(R, dp, C), (1, 0, 2))
    vm = pl.BlockSpec(memory_space=pltpu.VMEM)
    anyw = pl.BlockSpec(memory_space=pl.ANY)
    dma = pltpu.SemaphoreType.DMA
    loss, gh, gw = pl.pallas_call(
        functools.partial(kernel, (dp, T, nA, nB, sliced)),
        out_shape=(
            jax.ShapeDtypeStruct((8, 128), F32),
            jax.ShapeDtypeStruct((R, D // T), F32),
            jax.ShapeDtypeStruct((C, V), F32),
        ),
        in_specs=[anyw, anyw, anyw, vm, vm],
        out_specs=(vm, vm, vm),
        scratch_shapes=[
            pltpu.VMEM((R, D), BF16),
            pltpu.VMEM((D, V), BF16),
            pltpu.VMEM((R, V), F32),
            pltpu.VMEM((R, 128), F32),
            pltpu.VMEM((T, 8, R), F32),
            pltpu.VMEM((dp, G8 + 8, 128), F32),
            pltpu.VMEM((dp, 8, 128), F32),
            pltpu.VMEM((dp, R, V), BF16),
            pltpu.VMEM((dp, R, C), BF16),
            pltpu.VMEM((T, R, D // T), BF16),
            dma((2, 8)),
            dma((dp,)), dma((dp,)),
            dma((dp,)), dma((dp,)),
            dma((T,)), dma((T,)),
            dma((T,)), dma((T,)),
            dma((T,)), dma((T,)),
            dma((dp,)), dma((dp,)),
            dma((T,)), dma((T,)),
            dma((2, dp)), dma((nB, dp)), dma((dp,)),
        ],
        compiler_params=pltpu.CompilerParams(
            collective_id=0, has_side_effects=True, vmem_limit_bytes=63 * 1024 * 1024
        ),
    )(hidden, hsrc, head_weight, rows, info)
    return (loss[0, 0], gh, gw)


def solution(mesh):
    return jax.shard_map(
        shards,
        mesh=mesh,
        in_specs=(
            P("dp", None),
            P(None, "tensor"),
            P("dp"),
            P("dp"),
            P("dp"),
            P("dp"),
            P("dp"),
            P(),
        ),
        out_specs=(P(), P("dp", "tensor"), P("dp", "tensor")),
        check_vma=False,
    )
```

```python
import functools

import jax
import jax.numpy as jnp
from jax import lax
from jax.experimental import pallas as pl
from jax.experimental.pallas import tpu as pltpu
from jax.sharding import PartitionSpec as P

GROUP = 16
clip_low = 0.2
clip_high = 0.28
MESH = pl.DeviceIdType.MESH
F32 = jnp.float32
BF16 = jnp.bfloat16


def kernel(cfg, hidden, hsrc, w, tok_i, old_i, rew_i, len_i, gid_i, scale_i, loss_o, gh_o, gw_o,
           hid_v, w_v, logits, cols, rows, stats, info, info_all, loss_all, lg_all, hcol, rs_recv,
           ld, s_info, r_info, s_hid, r_hid, s_x, r_x, s_d, r_d, s_st, r_st,
           s_loss, r_loss, s_rs, r_rs, s_a, s_b, r_lg, s_t):
    dp, T, nA, nB, sliced = cfg
    R, D = hid_v.shape
    V = w_v.shape[1]
    Q = R // T
    C = D // dp
    CT = D // T
    nX = T // 2
    NK = 8
    KC = D // NK
    me = lax.axis_index("dp")
    t = lax.axis_index("tensor")
    a, b = me // nB, me % nB
    x, c = t // 2, t % 2

    def rcopy(src, dst, ss, rs, dev):
        return pltpu.make_async_remote_copy(
            src_ref=src, dst_ref=dst, send_sem=ss, recv_sem=rs, device_id=dev, device_id_type=MESH
        )

    def load_h(k):
        s = pl.ds(pl.multiple_of(k * KC, KC), KC)
        return pltpu.make_async_copy(hidden.at[:, s], hid_v.at[:, s], ld.at[0, k])

    def load_w(k):
        s = pl.ds(pl.multiple_of(k * KC, KC), KC)
        return pltpu.make_async_copy(w.at[s], w_v.at[s], ld.at[1, k])

    for k in range(NK):
        load_h(k).start()
        load_w(k).start()

    rolls = rew_i.shape[1]
    per_roll = R // rolls
    G8 = info.shape[0]
    reward_row = rew_i[...].astype(F32)
    length_row = len_i[...].astype(F32)
    group_row = gid_i[...].astype(F32)
    group_of = (lax.broadcasted_iota(jnp.int32, (G8, rolls), 0).astype(F32) == group_row).astype(F32)
    local_wins = jnp.sum(group_of * reward_row, axis=1, keepdims=True)
    local_lens = jnp.sum(group_of * length_row, axis=1, keepdims=True)
    glane = lax.broadcasted_iota(jnp.int32, (G8, 128), 1)
    info[...] = jnp.where(glane == 0, local_wins, jnp.where(glane == 1, local_lens, 0.0))
    diag = (
        lax.broadcasted_iota(jnp.int32, (rolls, rolls), 0) == lax.broadcasted_iota(jnp.int32, (rolls, rolls), 1)
    ).astype(F32)
    first = lax.broadcasted_iota(jnp.int32, (rolls, R), 0) * per_roll
    place = lax.broadcasted_iota(jnp.int32, (rolls, R), 1) - first
    mine = jnp.logical_and(place >= 0, place < per_roll).astype(F32)

    def spread_row(row):
        column = jnp.sum(diag * row, axis=1, keepdims=True)
        return jnp.sum(mine * column, axis=0, keepdims=True)

    place_row = jnp.sum(mine * place.astype(F32), axis=0, keepdims=True)
    rows[...] = jnp.concatenate(
        [
            tok_i[...].astype(F32), old_i[...], spread_row(group_row), spread_row(reward_row),
            (place_row < spread_row(length_row)).astype(F32), jnp.zeros((3, R), F32),
        ],
        axis=0,
    )

    barrier = pltpu.get_barrier_semaphore()
    for d in range(1, dp):
        pl.semaphore_signal(barrier, inc=1, device_id={"dp": (me + d) % dp}, device_id_type=MESH)
    for d in range(1, T):
        pl.semaphore_signal(barrier, inc=1, device_id={"tensor": (t + d) % T}, device_id_type=MESH)
    pl.semaphore_wait(barrier, dp - 1 + T - 1)

    def qrows(q):
        return pl.ds(pl.multiple_of(q * Q, Q), Q)

    def hslice(j):
        if sliced:
            return hsrc.at[qrows(t), pl.ds(pl.multiple_of(j * C, C), C)]
        return hsrc.at[j, qrows(t), :]

    def c_info(d):
        j = (me + d) % dp
        return rcopy(info, info_all.at[me], s_info.at[d], r_info.at[me], {"dp": j})

    def c_hid(d):
        j = (me + d) % dp
        return rcopy(hslice(j), hcol.at[me, qrows(t), :], s_hid.at[d], r_hid.at[me], {"dp": j})

    for d in range(1, dp):
        c_info(d).start()
    for d in range(1, dp):
        c_hid(d).start()
    own_hid = pltpu.make_async_copy(hslice(me), hcol.at[me, qrows(t), :], s_hid.at[0])
    own_hid.start()
    info_all[me] = info[...]

    pad = jnp.zeros((128 - rows.shape[0], R), F32)
    cols[...] = jnp.transpose(jnp.concatenate([rows[...], pad], axis=0))

    logits[...] = jnp.zeros_like(logits)

    @pl.loop(0, NK)
    def _(k):
        s = pl.ds(pl.multiple_of(k * KC, KC), KC)
        load_h(k).wait()
        load_w(k).wait()
        logits[...] += jnp.dot(hid_v[:, s], w_v[s, :], preferred_element_type=F32)

    RC = 32
    lane = lax.broadcasted_iota(jnp.int32, (RC, 128), 1)
    vcol = lax.broadcasted_iota(jnp.int32, (RC, V), 1).astype(F32) + (t * V).astype(F32)

    @pl.loop(0, R // RC)
    def _(n):
        r = pl.ds(pl.multiple_of(n * RC, RC), RC)
        lo = logits[r, :]
        tok = cols[r, 0:1]
        top = jnp.max(lo, axis=1, keepdims=True)
        target = jnp.sum(jnp.where(vcol == tok, lo, 0.0), axis=1, keepdims=True)
        e = jnp.exp(lo - top)
        total = jnp.sum(e, axis=1, keepdims=True)
        logits[r, :] = e
        cols[r, :] = jnp.where(
            lane == 0, tok, jnp.where(lane == 1, top, jnp.where(lane == 2, total, jnp.where(lane == 3, target, 0.0)))
        )

    stats[t] = jnp.transpose(cols[...])[0:8, :]

    def c_st(d):
        return rcopy(stats.at[t], stats.at[t], s_st.at[d], r_st.at[t], {"tensor": (t + d) % T})

    for d in range(1, T):
        c_st(d).start()
    for d in range(1, dp):
        i = (me + d) % dp
        rcopy(info, info_all.at[i], s_info.at[d], r_info.at[i], {"dp": i}).wait_recv()
    wins2 = info_all[0]
    for i in range(1, dp):
        wins2 = wins2 + info_all[i]
    wins = wins2[0:G8, 0:1]
    lens = wins2[0:G8, 1:2]
    alive = jnp.logical_and(wins > 0.5, wins < GROUP - 0.5).astype(F32)
    center = wins / GROUP
    spread = jnp.where(alive > 0.5, jnp.sqrt(wins * (GROUP - wins)) / GROUP, 1.0)
    token_count = jnp.sum(alive * lens, axis=0, keepdims=True)
    divisor = jnp.maximum(token_count, 1.0)
    factor = scale_i[...] / divisor
    old = rows[1:2, :]
    gid = rows[2:3, :]
    rew = rows[3:4, :]
    inside = rows[4:5, :]
    member = (lax.broadcasted_iota(jnp.int32, (G8, R), 0).astype(F32) == gid).astype(F32)
    roll_alive = jnp.sum(member * alive, axis=0, keepdims=True)
    roll_center = jnp.sum(member * center, axis=0, keepdims=True)
    roll_spread = jnp.sum(member * spread, axis=0, keepdims=True)
    adv = roll_alive * (rew - roll_center) / roll_spread
    weight = roll_alive * inside

    for d in range(1, T):
        i = (t + d) % T
        rcopy(stats.at[i], stats.at[i], s_st.at[d], r_st.at[i], {"tensor": i}).wait_recv()
    top = stats[0, 1:2, :]
    for i in range(1, T):
        top = jnp.maximum(top, stats[i, 1:2, :])
    total = jnp.zeros_like(top)
    target = jnp.zeros_like(top)
    for i in range(T):
        total = total + stats[i, 2:3, :] * jnp.exp(stats[i, 1:2, :] - top)
        target = target + stats[i, 3:4, :]
    log_prob = target - top - jnp.log(total)
    ratio = jnp.exp(log_prob - old)
    clipped = jnp.clip(ratio, 1.0 - clip_low, 1.0 + clip_high)
    token_loss = -jnp.minimum(ratio * adv, clipped * adv)
    active = ratio * adv <= clipped * adv
    coef = jnp.where(active, -adv * ratio, 0.0) * weight * factor
    mytop = stats[t][1:2, :]
    scale = jnp.exp(mytop - top) / total
    loss_all[me] = jnp.broadcast_to(jnp.sum(weight * token_loss, axis=1, keepdims=True), (8, 128))
    cols[...] = jnp.transpose(
        jnp.concatenate([rows[0:1, :], coef, scale, jnp.zeros((125, R), F32)], axis=0)
    )

    @pl.loop(0, R // RC)
    def _(n):
        r = pl.ds(pl.multiple_of(n * RC, RC), RC)
        hit = jnp.where(vcol == cols[r, 0:1], 1.0, 0.0)
        lg_all[me, r, :] = (cols[r, 1:2] * (hit - logits[r, :] * cols[r, 2:3])).astype(BF16)

    H = R // 2
    swap = nB == 2 and nA % 2 == 0
    twin = a + 1 - 2 * (a % 2)

    def half(j, h):
        return lg_all.at[j, pl.ds(h * H, H), :]

    def c_up(j, h):
        return rcopy(half(j, h), half(j, h), s_a.at[0, j, h], r_lg.at[j, h], {"dp": me + nB})

    def c_down(j, h):
        return rcopy(half(j, h), half(j, h), s_a.at[1, j, h], r_lg.at[j, h], {"dp": me - nB})

    def c_b(j, h, d):
        return rcopy(half(j, h), half(j, h), s_b.at[d, j, h], r_lg.at[j, h], {"dp": a * nB + (b + d) % nB})

    def c_twin():
        j = a * nB + (b + 1) % nB
        return rcopy(half(j, 0), half(j, 0), s_t, r_lg.at[j, 0], {"dp": twin * nB + b})

    def recv_lg(j, h):
        rcopy(half(j, h), half(j, h), s_a.at[0, j, h], r_lg.at[j, h], {"dp": (me + 1) % dp}).wait_recv()

    def each_b(j, h, act):
        def go():
            for d in range(1, nB):
                act(c_b(j, h, d))

        if swap and h == 0:
            pl.when(j != twin * nB + b)(go)
        else:
            go()

    def start(copy):
        copy.start()

    def done(copy):
        copy.wait_send()

    for h in range(2):
        @pl.when(a < nA - 1)
        def _():
            c_up(me, h).start()

        @pl.when(a > 0)
        def _():
            c_down(me, h).start()

        each_b(me, h, start)

    def c_loss(d):
        return rcopy(loss_all.at[me], loss_all.at[me], s_loss.at[d], r_loss.at[me], {"dp": (me + d) % dp})

    for d in range(1, dp):
        c_loss(d).start()

    GC = 640 if CT % 640 == 0 else CT
    per = CT // GC

    def gh_dot(col0):
        return lax.dot_general(
            lg_all[me], w_v[pl.ds(col0, GC), :], (((1,), (1,)), ((), ())), preferred_element_type=F32
        )

    other = 2 * x + 1 - c

    def gcols(shard):
        return hid_v.at[:, pl.ds(pl.multiple_of(shard * CT, CT), CT)]

    def c_pair(xx):
        return rcopy(gcols(2 * xx + 1 - c), rs_recv.at[xx], s_rs.at[xx], r_rs.at[xx], {"tensor": other})

    def wait_pair(xx):
        rcopy(gcols(2 * xx + c), rs_recv.at[xx], s_rs.at[xx], r_rs.at[xx], {"tensor": other}).wait_recv()

    def c_rs(d):
        peer = ((x + d) % nX) * 2 + c
        return rcopy(gcols(peer), rs_recv.at[nX + x], s_rs.at[nX + d], r_rs.at[nX + x], {"tensor": peer})

    @pl.loop(0, nX * per)
    def _(n):
        col0 = pl.multiple_of((2 * (n // per) + 1 - c) * CT + (n % per) * GC, GC)
        hid_v[:, pl.ds(col0, GC)] = gh_dot(col0).astype(BF16)

    for xx in range(nX):
        c_pair(xx).start()

    @pl.loop(0, per)
    def _(n):
        off = pl.multiple_of(n * GC, GC)
        gh_o[:, pl.ds(off, GC)] = gh_dot(pl.multiple_of(t * CT + off, GC))

    for xx in range(nX):
        wait_pair(xx)

    @pl.loop(0, (nX - 1) * per)
    def _(n):
        xx = (x + 1 + n // per) % nX
        off = pl.multiple_of((n % per) * GC, GC)
        col0 = pl.multiple_of((2 * xx + c) * CT + off, GC)
        hid_v[:, pl.ds(col0, GC)] = (gh_dot(col0) + rs_recv[xx, :, pl.ds(off, GC)].astype(F32)).astype(BF16)

    own_hid.wait()
    for d in range(1, dp):
        i = (me + d) % dp
        rcopy(hslice(i), hcol.at[i, qrows(t), :], s_hid.at[d], r_hid.at[i], {"dp": i}).wait_recv()

    def c_x(d):
        q = hcol.at[:, qrows(t), :]
        return rcopy(q, q, s_x.at[d], r_x.at[x], {"tensor": ((x + d) % nX) * 2 + c})

    def c_d(xx):
        q = hcol.at[:, qrows(2 * xx + c), :]
        return rcopy(q, q, s_d.at[xx], r_d.at[xx], {"tensor": 2 * x + 1 - c})

    for d in range(1, nX):
        c_x(d).start()
    c_d(x).start()

    for d in range(1, nX):
        c_rs(d).start()

    def relay(s):
        for h in range(2):
            @pl.when(a >= s)
            def _():
                j = me - s * nB
                recv_lg(j, h)

                @pl.when(a < nA - 1)
                def _():
                    c_up(j, h).start()

                each_b(j, h, start)

            @pl.when(a + s < nA)
            def _():
                j = me + s * nB
                recv_lg(j, h)

                @pl.when(a > 0)
                def _():
                    c_down(j, h).start()

                each_b(j, h, start)

    def gw_add(j):
        gw_o[...] += lax.dot_general(
            hcol[j], lg_all[j], (((0,), (0,)), ((), ())), preferred_element_type=F32
        )

    gw_o[...] = jnp.zeros_like(gw_o)

    def add_steps(items):
        for s, d in items:
            @pl.loop(0, 1 if s == 0 else 2)
            def _(k):
                aa = a + (2 * k - 1) * s
                j = aa * nB + (b + d) % nB

                @pl.when(jnp.logical_and(aa >= 0, aa < nA))
                def _():
                    if d > 0:
                        if not (swap and s == 0):
                            recv_lg(j, 0)
                        recv_lg(j, 1)
                    gw_add(j)

    relay(1)
    relay(2)
    if swap:
        recv_lg(a * nB + (b + 1) % nB, 0)
        c_twin().start()
    for d in range(1, nX):
        xx = (x + d) % nX
        q = hcol.at[:, qrows(2 * xx + c), :]
        rcopy(q, q, s_x.at[d], r_x.at[xx], {"tensor": 2 * xx + c}).wait_recv()
        c_d(xx).start()
    for xx in range(nX):
        q = hcol.at[:, qrows(2 * xx + 1 - c), :]
        rcopy(q, q, s_d.at[xx], r_d.at[xx], {"tensor": 2 * x + 1 - c}).wait_recv()
    add_steps([(0, 0), (1, 0), (2, 0)] + [(0, d) for d in range(1, nB)])
    for s in range(3, nA):
        relay(s)
        add_steps([(s, 0)])
    for s in range(1, nA - 1):
        add_steps([(s, d) for d in range(1, nB)])

    for d in range(1, nX):
        xx = (x + d) % nX
        rcopy(gcols(t), rs_recv.at[nX + xx], s_rs.at[nX + d], r_rs.at[nX + xx], {"tensor": 2 * xx + c}).wait_recv()

    @pl.loop(0, R // RC)
    def _(n):
        r = pl.ds(pl.multiple_of(n * RC, RC), RC)
        acc = gh_o[r, :] + rs_recv[x, r, :].astype(F32)
        for d in range(1, nX):
            acc = acc + rs_recv[nX + (x + d) % nX, r, :].astype(F32)
        gh_o[r, :] = acc

    for d in range(1, dp):
        i = (me + d) % dp
        rcopy(loss_all.at[i], loss_all.at[i], s_loss.at[d], r_loss.at[i], {"dp": i}).wait_recv()
    loss = loss_all[0]
    for i in range(1, dp):
        loss = loss + loss_all[i]
    loss_o[...] = loss[0:1, 0:1] / divisor

    add_steps([(nA - 1, d) for d in range(1, nB)])

    for d in range(1, dp):
        c_info(d).wait_send()
        c_hid(d).wait_send()
        c_loss(d).wait_send()
    for d in range(1, T):
        c_st(d).wait_send()
    for d in range(1, nX):
        c_x(d).wait_send()
        c_rs(d).wait_send()
    for xx in range(nX):
        c_d(xx).wait_send()
        c_pair(xx).wait_send()
    if swap:
        c_twin().wait_send()
    for s in range(nA):
        for h in range(2):
            @pl.when(a >= s)
            def _():
                j = me - s * nB

                @pl.when(a < nA - 1)
                def _():
                    c_up(j, h).wait_send()

                each_b(j, h, done)

            if s > 0:
                @pl.when(a + s < nA)
                def _():
                    j = me + s * nB

                    @pl.when(a > 0)
                    def _():
                        c_down(j, h).wait_send()

                    each_b(j, h, done)

    for h in range(2):
        @pl.when(a > 0)
        def _():
            c_down(me, h).wait_send()


def shards(hidden, head_weight, token_ids, old_logprob, rewards, lengths, group_ids, loss_scale):
    R, D = hidden.shape
    V = head_weight.shape[1]
    rolls = rewards.shape[0]
    dp = lax.axis_size("dp")
    T = lax.axis_size("tensor")
    nA = 4 if dp % 4 == 0 else dp
    nB = dp // nA
    groups = rolls * dp // GROUP
    G8 = -(-groups // 8) * 8
    C = D // dp
    sliced = C % 128 == 0
    if sliced:
        hsrc = hidden
    else:
        hsrc = jnp.transpose(hidden.reshape(R, dp, C), (1, 0, 2))
    vm = pl.BlockSpec(memory_space=pltpu.VMEM)
    anyw = pl.BlockSpec(memory_space=pl.ANY)
    dma = pltpu.SemaphoreType.DMA
    loss, gh, gw = pl.pallas_call(
        functools.partial(kernel, (dp, T, nA, nB, sliced)),
        out_shape=(
            jax.ShapeDtypeStruct((1, 1), F32),
            jax.ShapeDtypeStruct((R, D // T), F32),
            jax.ShapeDtypeStruct((C, V), F32),
        ),
        in_specs=[anyw] * 3 + [vm] * 6,
        out_specs=(vm, vm, vm),
        scratch_shapes=[
            pltpu.VMEM((R, D), BF16),
            pltpu.VMEM((D, V), BF16),
            pltpu.VMEM((R, V), F32),
            pltpu.VMEM((R, 128), F32),
            pltpu.VMEM((8, R), F32),
            pltpu.VMEM((T, 8, R), F32),
            pltpu.VMEM((G8, 128), F32),
            pltpu.VMEM((dp, G8, 128), F32),
            pltpu.VMEM((dp, 8, 128), F32),
            pltpu.VMEM((dp, R, V), BF16),
            pltpu.VMEM((dp, R, C), BF16),
            pltpu.VMEM((T, R, D // T), BF16),
            dma((2, 8)),
            dma((dp,)), dma((dp,)),
            dma((dp,)), dma((dp,)),
            dma((T,)), dma((T,)),
            dma((T,)), dma((T,)),
            dma((T,)), dma((T,)),
            dma((dp,)), dma((dp,)),
            dma((T,)), dma((T,)),
            dma((2, dp, 2)), dma((nB, dp, 2)), dma((dp, 2)), dma(()),
        ],
        compiler_params=pltpu.CompilerParams(
            collective_id=0, has_side_effects=True, vmem_limit_bytes=63 * 1024 * 1024
        ),
    )(
        hidden, hsrc, head_weight, token_ids.reshape(1, R), old_logprob.reshape(1, R),
        rewards.reshape(1, rolls), lengths.reshape(1, rolls), group_ids.reshape(1, rolls),
        loss_scale.reshape(1, 1),
    )
    return (loss.reshape(()), gh, gw)


def solution(mesh):
    return jax.shard_map(
        shards,
        mesh=mesh,
        in_specs=(
            P("dp", None),
            P(None, "tensor"),
            P("dp"),
            P("dp"),
            P("dp"),
            P("dp"),
            P("dp"),
            P(),
        ),
        out_specs=(P(), P("dp", "tensor"), P("dp", "tensor")),
        check_vma=False,
    )
```

```python
import functools

import jax
import jax.numpy as jnp
from jax import lax
from jax.experimental import pallas as pl
from jax.experimental.pallas import tpu as pltpu
from jax.sharding import PartitionSpec as P

GROUP = 16
clip_low = 0.2
clip_high = 0.28
MESH = pl.DeviceIdType.MESH
F32 = jnp.float32
BF16 = jnp.bfloat16


def kernel(cfg, hidden, hsrc, w, tok_i, old_i, rew_i, len_i, gid_i, scale_i, loss_o, gh_o, gw_o,
           hid_v, w_v, logits, cols, rows, stats, info, info_all, loss_all, lg_all, hcol, rs_recv,
           ld, s_info, r_info, s_hid, r_hid, s_x, r_x, s_d, r_d, s_st, r_st,
           s_loss, r_loss, s_rs, r_rs, s_a, s_b, r_lg, s_t):
    dp, T, nA, nB, sliced = cfg
    R, D = hid_v.shape
    V = w_v.shape[1]
    Q = R // T
    C = D // dp
    CT = D // T
    nX = T // 2
    NK = 8
    KC = D // NK
    me = lax.axis_index("dp")
    t = lax.axis_index("tensor")
    a, b = me // nB, me % nB
    x, c = t // 2, t % 2

    def rcopy(src, dst, ss, rs, dev):
        return pltpu.make_async_remote_copy(
            src_ref=src, dst_ref=dst, send_sem=ss, recv_sem=rs, device_id=dev, device_id_type=MESH
        )

    def load_h(k):
        s = pl.ds(pl.multiple_of(k * KC, KC), KC)
        return pltpu.make_async_copy(hidden.at[:, s], hid_v.at[:, s], ld.at[0, k])

    def load_w(k):
        s = pl.ds(pl.multiple_of(k * KC, KC), KC)
        return pltpu.make_async_copy(w.at[s], w_v.at[s], ld.at[1, k])

    for k in range(NK):
        load_h(k).start()
        load_w(k).start()

    rolls = rew_i.shape[1]
    per_roll = R // rolls
    G8 = info.shape[0]
    reward_row = rew_i[...].astype(F32)
    length_row = len_i[...].astype(F32)
    group_row = gid_i[...].astype(F32)
    group_of = (lax.broadcasted_iota(jnp.int32, (G8, rolls), 0).astype(F32) == group_row).astype(F32)
    local_wins = jnp.sum(group_of * reward_row, axis=1, keepdims=True)
    local_lens = jnp.sum(group_of * length_row, axis=1, keepdims=True)
    glane = lax.broadcasted_iota(jnp.int32, (G8, 128), 1)
    info[...] = jnp.where(glane == 0, local_wins, jnp.where(glane == 1, local_lens, 0.0))
    diag = (
        lax.broadcasted_iota(jnp.int32, (rolls, rolls), 0) == lax.broadcasted_iota(jnp.int32, (rolls, rolls), 1)
    ).astype(F32)
    first = lax.broadcasted_iota(jnp.int32, (rolls, R), 0) * per_roll
    place = lax.broadcasted_iota(jnp.int32, (rolls, R), 1) - first
    mine = jnp.logical_and(place >= 0, place < per_roll).astype(F32)

    def spread_row(row):
        column = jnp.sum(diag * row, axis=1, keepdims=True)
        return jnp.sum(mine * column, axis=0, keepdims=True)

    place_row = jnp.sum(mine * place.astype(F32), axis=0, keepdims=True)
    rows[...] = jnp.concatenate(
        [
            tok_i[...].astype(F32), old_i[...], spread_row(group_row), spread_row(reward_row),
            (place_row < spread_row(length_row)).astype(F32), jnp.zeros((3, R), F32),
        ],
        axis=0,
    )

    barrier = pltpu.get_barrier_semaphore()
    for d in range(1, dp):
        pl.semaphore_signal(barrier, inc=1, device_id={"dp": (me + d) % dp}, device_id_type=MESH)
    for d in range(1, T):
        pl.semaphore_signal(barrier, inc=1, device_id={"tensor": (t + d) % T}, device_id_type=MESH)
    pl.semaphore_wait(barrier, dp - 1 + T - 1)

    def qrows(q):
        return pl.ds(pl.multiple_of(q * Q, Q), Q)

    def hslice(j):
        if sliced:
            return hsrc.at[qrows(t), pl.ds(pl.multiple_of(j * C, C), C)]
        return hsrc.at[j, qrows(t), :]

    def c_info(d):
        j = (me + d) % dp
        return rcopy(info, info_all.at[me], s_info.at[d], r_info.at[me], {"dp": j})

    def c_hid(d):
        j = (me + d) % dp
        return rcopy(hslice(j), hcol.at[me, qrows(t), :], s_hid.at[d], r_hid.at[me], {"dp": j})

    for d in range(1, dp):
        c_info(d).start()
    for d in range(1, dp):
        c_hid(d).start()
    own_hid = pltpu.make_async_copy(hslice(me), hcol.at[me, qrows(t), :], s_hid.at[0])
    own_hid.start()
    info_all[me] = info[...]

    pad = jnp.zeros((128 - rows.shape[0], R), F32)
    cols[...] = jnp.transpose(jnp.concatenate([rows[...], pad], axis=0))

    H = R // 2
    swap = nB == 2 and nA % 2 == 0
    twin = a + 1 - 2 * (a % 2)

    def half(j, h):
        return lg_all.at[j, pl.ds(h * H, H), :]

    def c_up(j, h):
        return rcopy(half(j, h), half(j, h), s_a.at[0, j, h], r_lg.at[j, h], {"dp": me + nB})

    def c_down(j, h):
        return rcopy(half(j, h), half(j, h), s_a.at[1, j, h], r_lg.at[j, h], {"dp": me - nB})

    def c_b(j, h, d):
        return rcopy(half(j, h), half(j, h), s_b.at[d, j, h], r_lg.at[j, h], {"dp": a * nB + (b + d) % nB})

    def c_twin():
        j = a * nB + (b + 1) % nB
        return rcopy(half(j, 0), half(j, 0), s_t, r_lg.at[j, 0], {"dp": twin * nB + b})

    def recv_lg(j, h):
        rcopy(half(j, h), half(j, h), s_a.at[0, j, h], r_lg.at[j, h], {"dp": (me + 1) % dp}).wait_recv()

    def each_b(j, h, act):
        def go():
            for d in range(1, nB):
                act(c_b(j, h, d))

        if swap and h == 0:
            pl.when(j != twin * nB + b)(go)
        else:
            go()

    def start(copy):
        copy.start()

    def done(copy):
        copy.wait_send()

    logits[...] = jnp.zeros_like(logits)
    RC = 32
    lane = lax.broadcasted_iota(jnp.int32, (RC, 128), 1)
    vcol = lax.broadcasted_iota(jnp.int32, (RC, V), 1).astype(F32) + (t * V).astype(F32)
    loss_sum = jnp.zeros((1, 1), F32)

    def c_st(h, d):
        return rcopy(stats.at[h, t], stats.at[h, t], s_st.at[h, d], r_st.at[h, t], {"tensor": (t + d) % T})

    for h in range(2):
        rh = pl.ds(h * H, H)
        hs = slice(h * H, (h + 1) * H)

        @pl.loop(0, NK)
        def _(k):
            s = pl.ds(pl.multiple_of(k * KC, KC), KC)
            if h == 0:
                load_h(k).wait()
                load_w(k).wait()
            logits[rh, :] += jnp.dot(hid_v[rh, s], w_v[s, :], preferred_element_type=F32)

        @pl.loop(0, H // RC)
        def _(n):
            r = pl.ds(pl.multiple_of(h * H + n * RC, RC), RC)
            lo = logits[r, :]
            tok = cols[r, 0:1]
            top = jnp.max(lo, axis=1, keepdims=True)
            target = jnp.sum(jnp.where(vcol == tok, lo, 0.0), axis=1, keepdims=True)
            e = jnp.exp(lo - top)
            total = jnp.sum(e, axis=1, keepdims=True)
            logits[r, :] = e
            cols[r, :] = jnp.where(
                lane == 0, tok, jnp.where(lane == 1, top, jnp.where(lane == 2, total, jnp.where(lane == 3, target, 0.0)))
            )

        stats[h, t] = jnp.transpose(cols[rh, :])[0:8, :]
        for d in range(1, T):
            c_st(h, d).start()
        if h == 0:
            for d in range(1, dp):
                i = (me + d) % dp
                rcopy(info, info_all.at[i], s_info.at[d], r_info.at[i], {"dp": i}).wait_recv()
            wins2 = info_all[0]
            for i in range(1, dp):
                wins2 = wins2 + info_all[i]
            wins = wins2[0:G8, 0:1]
            lens = wins2[0:G8, 1:2]
            alive = jnp.logical_and(wins > 0.5, wins < GROUP - 0.5).astype(F32)
            center = wins / GROUP
            spread = jnp.where(alive > 0.5, jnp.sqrt(wins * (GROUP - wins)) / GROUP, 1.0)
            token_count = jnp.sum(alive * lens, axis=0, keepdims=True)
            divisor = jnp.maximum(token_count, 1.0)
            factor = scale_i[...] / divisor
            old = rows[1:2, :]
            gid = rows[2:3, :]
            rew = rows[3:4, :]
            inside = rows[4:5, :]
            member = (lax.broadcasted_iota(jnp.int32, (G8, R), 0).astype(F32) == gid).astype(F32)
            roll_alive = jnp.sum(member * alive, axis=0, keepdims=True)
            roll_center = jnp.sum(member * center, axis=0, keepdims=True)
            roll_spread = jnp.sum(member * spread, axis=0, keepdims=True)
            adv = roll_alive * (rew - roll_center) / roll_spread
            weight = roll_alive * inside

        for d in range(1, T):
            i = (t + d) % T
            rcopy(stats.at[h, i], stats.at[h, i], s_st.at[h, d], r_st.at[h, i], {"tensor": i}).wait_recv()
        top = stats[h, 0, 1:2, :]
        for i in range(1, T):
            top = jnp.maximum(top, stats[h, i, 1:2, :])
        total = jnp.zeros_like(top)
        target = jnp.zeros_like(top)
        for i in range(T):
            total = total + stats[h, i, 2:3, :] * jnp.exp(stats[h, i, 1:2, :] - top)
            target = target + stats[h, i, 3:4, :]
        adv_h, weight_h = adv[:, hs], weight[:, hs]
        log_prob = target - top - jnp.log(total)
        ratio = jnp.exp(log_prob - old[:, hs])
        clipped = jnp.clip(ratio, 1.0 - clip_low, 1.0 + clip_high)
        token_loss = -jnp.minimum(ratio * adv_h, clipped * adv_h)
        active = ratio * adv_h <= clipped * adv_h
        coef = jnp.where(active, -adv_h * ratio, 0.0) * weight_h * factor
        mytop = stats[h, t][1:2, :]
        scale = jnp.exp(mytop - top) / total
        loss_sum = loss_sum + jnp.sum(weight_h * token_loss, axis=1, keepdims=True)
        cols[rh, :] = jnp.transpose(
            jnp.concatenate([rows[0:1, hs], coef, scale, jnp.zeros((125, H), F32)], axis=0)
        )

        @pl.loop(0, H // RC)
        def _(n):
            r = pl.ds(pl.multiple_of(h * H + n * RC, RC), RC)
            hit = jnp.where(vcol == cols[r, 0:1], 1.0, 0.0)
            lg_all[me, r, :] = (cols[r, 1:2] * (hit - logits[r, :] * cols[r, 2:3])).astype(BF16)

        @pl.when(a < nA - 1)
        def _():
            c_up(me, h).start()

        @pl.when(a > 0)
        def _():
            c_down(me, h).start()

        each_b(me, h, start)

    loss_all[me] = jnp.broadcast_to(loss_sum, (8, 128))

    def c_loss(d):
        return rcopy(loss_all.at[me], loss_all.at[me], s_loss.at[d], r_loss.at[me], {"dp": (me + d) % dp})

    for d in range(1, dp):
        c_loss(d).start()

    GC = 640 if CT % 640 == 0 else CT
    per = CT // GC

    def gh_dot(col0):
        return lax.dot_general(
            lg_all[me], w_v[pl.ds(col0, GC), :], (((1,), (1,)), ((), ())), preferred_element_type=F32
        )

    other = 2 * x + 1 - c

    def gcols(shard):
        return hid_v.at[:, pl.ds(pl.multiple_of(shard * CT, CT), CT)]

    def c_pair(xx):
        return rcopy(gcols(2 * xx + 1 - c), rs_recv.at[xx], s_rs.at[xx], r_rs.at[xx], {"tensor": other})

    def wait_pair(xx):
        rcopy(gcols(2 * xx + c), rs_recv.at[xx], s_rs.at[xx], r_rs.at[xx], {"tensor": other}).wait_recv()

    def c_rs(d):
        peer = ((x + d) % nX) * 2 + c
        return rcopy(gcols(peer), rs_recv.at[nX + x], s_rs.at[nX + d], r_rs.at[nX + x], {"tensor": peer})

    @pl.loop(0, nX * per)
    def _(n):
        col0 = pl.multiple_of((2 * (n // per) + 1 - c) * CT + (n % per) * GC, GC)
        hid_v[:, pl.ds(col0, GC)] = gh_dot(col0).astype(BF16)

    for xx in range(nX):
        c_pair(xx).start()

    @pl.loop(0, per)
    def _(n):
        off = pl.multiple_of(n * GC, GC)
        gh_o[:, pl.ds(off, GC)] = gh_dot(pl.multiple_of(t * CT + off, GC))

    for xx in range(nX):
        wait_pair(xx)

    @pl.loop(0, (nX - 1) * per)
    def _(n):
        xx = (x + 1 + n // per) % nX
        off = pl.multiple_of((n % per) * GC, GC)
        col0 = pl.multiple_of((2 * xx + c) * CT + off, GC)
        hid_v[:, pl.ds(col0, GC)] = (gh_dot(col0) + rs_recv[xx, :, pl.ds(off, GC)].astype(F32)).astype(BF16)

    own_hid.wait()
    for d in range(1, dp):
        i = (me + d) % dp
        rcopy(hslice(i), hcol.at[i, qrows(t), :], s_hid.at[d], r_hid.at[i], {"dp": i}).wait_recv()

    def c_x(d):
        q = hcol.at[:, qrows(t), :]
        return rcopy(q, q, s_x.at[d], r_x.at[x], {"tensor": ((x + d) % nX) * 2 + c})

    def c_d(xx):
        q = hcol.at[:, qrows(2 * xx + c), :]
        return rcopy(q, q, s_d.at[xx], r_d.at[xx], {"tensor": 2 * x + 1 - c})

    for d in range(1, nX):
        c_x(d).start()
    c_d(x).start()

    for d in range(1, nX):
        c_rs(d).start()

    def relay(s):
        for h in range(2):
            @pl.when(a >= s)
            def _():
                j = me - s * nB
                recv_lg(j, h)

                @pl.when(a < nA - 1)
                def _():
                    c_up(j, h).start()

                each_b(j, h, start)

            @pl.when(a + s < nA)
            def _():
                j = me + s * nB
                recv_lg(j, h)

                @pl.when(a > 0)
                def _():
                    c_down(j, h).start()

                each_b(j, h, start)

    def gw_add(j):
        gw_o[...] += lax.dot_general(
            hcol[j], lg_all[j], (((0,), (0,)), ((), ())), preferred_element_type=F32
        )

    gw_o[...] = jnp.zeros_like(gw_o)

    def add_steps(items):
        for s, d in items:
            @pl.loop(0, 1 if s == 0 else 2)
            def _(k):
                aa = a + (2 * k - 1) * s
                j = aa * nB + (b + d) % nB

                @pl.when(jnp.logical_and(aa >= 0, aa < nA))
                def _():
                    if d > 0:
                        if not (swap and s == 0):
                            recv_lg(j, 0)
                        recv_lg(j, 1)
                    gw_add(j)

    relay(1)
    relay(2)
    if swap:
        recv_lg(a * nB + (b + 1) % nB, 0)
        c_twin().start()
    for d in range(1, nX):
        xx = (x + d) % nX
        q = hcol.at[:, qrows(2 * xx + c), :]
        rcopy(q, q, s_x.at[d], r_x.at[xx], {"tensor": 2 * xx + c}).wait_recv()
        c_d(xx).start()
    for xx in range(nX):
        q = hcol.at[:, qrows(2 * xx + 1 - c), :]
        rcopy(q, q, s_d.at[xx], r_d.at[xx], {"tensor": 2 * x + 1 - c}).wait_recv()
    add_steps([(0, 0), (1, 0), (2, 0)] + [(0, d) for d in range(1, nB)])
    for s in range(3, nA):
        relay(s)
        add_steps([(s, 0)])
    for s in range(1, nA - 1):
        add_steps([(s, d) for d in range(1, nB)])

    for d in range(1, nX):
        xx = (x + d) % nX
        rcopy(gcols(t), rs_recv.at[nX + xx], s_rs.at[nX + d], r_rs.at[nX + xx], {"tensor": 2 * xx + c}).wait_recv()

    @pl.loop(0, R // RC)
    def _(n):
        r = pl.ds(pl.multiple_of(n * RC, RC), RC)
        acc = gh_o[r, :] + rs_recv[x, r, :].astype(F32)
        for d in range(1, nX):
            acc = acc + rs_recv[nX + (x + d) % nX, r, :].astype(F32)
        gh_o[r, :] = acc

    for d in range(1, dp):
        i = (me + d) % dp
        rcopy(loss_all.at[i], loss_all.at[i], s_loss.at[d], r_loss.at[i], {"dp": i}).wait_recv()
    loss = loss_all[0]
    for i in range(1, dp):
        loss = loss + loss_all[i]
    loss_o[...] = loss[0:1, 0:1] / divisor

    add_steps([(nA - 1, d) for d in range(1, nB)])

    for d in range(1, dp):
        c_info(d).wait_send()
        c_hid(d).wait_send()
        c_loss(d).wait_send()
    for d in range(1, T):
        for h in range(2):
            c_st(h, d).wait_send()
    for d in range(1, nX):
        c_x(d).wait_send()
        c_rs(d).wait_send()
    for xx in range(nX):
        c_d(xx).wait_send()
        c_pair(xx).wait_send()
    if swap:
        c_twin().wait_send()
    for s in range(nA):
        for h in range(2):
            @pl.when(a >= s)
            def _():
                j = me - s * nB

                @pl.when(a < nA - 1)
                def _():
                    c_up(j, h).wait_send()

                each_b(j, h, done)

            if s > 0:
                @pl.when(a + s < nA)
                def _():
                    j = me + s * nB

                    @pl.when(a > 0)
                    def _():
                        c_down(j, h).wait_send()

                    each_b(j, h, done)

    for h in range(2):
        @pl.when(a > 0)
        def _():
            c_down(me, h).wait_send()


def shards(hidden, head_weight, token_ids, old_logprob, rewards, lengths, group_ids, loss_scale):
    R, D = hidden.shape
    V = head_weight.shape[1]
    rolls = rewards.shape[0]
    dp = lax.axis_size("dp")
    T = lax.axis_size("tensor")
    nA = 4 if dp % 4 == 0 else dp
    nB = dp // nA
    groups = rolls * dp // GROUP
    G8 = -(-groups // 8) * 8
    C = D // dp
    sliced = C % 128 == 0
    if sliced:
        hsrc = hidden
    else:
        hsrc = jnp.transpose(hidden.reshape(R, dp, C), (1, 0, 2))
    vm = pl.BlockSpec(memory_space=pltpu.VMEM)
    anyw = pl.BlockSpec(memory_space=pl.ANY)
    dma = pltpu.SemaphoreType.DMA
    loss, gh, gw = pl.pallas_call(
        functools.partial(kernel, (dp, T, nA, nB, sliced)),
        out_shape=(
            jax.ShapeDtypeStruct((1, 1), F32),
            jax.ShapeDtypeStruct((R, D // T), F32),
            jax.ShapeDtypeStruct((C, V), F32),
        ),
        in_specs=[anyw] * 3 + [vm] * 6,
        out_specs=(vm, vm, vm),
        scratch_shapes=[
            pltpu.VMEM((R, D), BF16),
            pltpu.VMEM((D, V), BF16),
            pltpu.VMEM((R, V), F32),
            pltpu.VMEM((R, 128), F32),
            pltpu.VMEM((8, R), F32),
            pltpu.VMEM((2, T, 8, R // 2), F32),
            pltpu.VMEM((G8, 128), F32),
            pltpu.VMEM((dp, G8, 128), F32),
            pltpu.VMEM((dp, 8, 128), F32),
            pltpu.VMEM((dp, R, V), BF16),
            pltpu.VMEM((dp, R, C), BF16),
            pltpu.VMEM((T, R, D // T), BF16),
            dma((2, 8)),
            dma((dp,)), dma((dp,)),
            dma((dp,)), dma((dp,)),
            dma((T,)), dma((T,)),
            dma((T,)), dma((T,)),
            dma((2, T)), dma((2, T)),
            dma((dp,)), dma((dp,)),
            dma((T,)), dma((T,)),
            dma((2, dp, 2)), dma((nB, dp, 2)), dma((dp, 2)), dma(()),
        ],
        compiler_params=pltpu.CompilerParams(
            collective_id=0, has_side_effects=True, vmem_limit_bytes=63 * 1024 * 1024
        ),
    )(
        hidden, hsrc, head_weight, token_ids.reshape(1, R), old_logprob.reshape(1, R),
        rewards.reshape(1, rolls), lengths.reshape(1, rolls), group_ids.reshape(1, rolls),
        loss_scale.reshape(1, 1),
    )
    return (loss.reshape(()), gh, gw)


def solution(mesh):
    return jax.shard_map(
        shards,
        mesh=mesh,
        in_specs=(
            P("dp", None),
            P(None, "tensor"),
            P("dp"),
            P("dp"),
            P("dp"),
            P("dp"),
            P("dp"),
            P(),
        ),
        out_specs=(P(), P("dp", "tensor"), P("dp", "tensor")),
        check_vma=False,
    )
```
